32 devices in a mesh: gx: 4 (over y, x), gy: 2 (over core), gz: 4 (over z).
Axes of the slice: x: 2, y: 2, z: 4, core: 2. Of those that a mesh axis runs over, the one named last changes fastest.
Arguments:
- right_side: float32 [81, 16, 16, 512], P(None, 'gx', 'gy', 'gz'), may hold values from -18 to 18
- cell_coef: float32 [16, 16, 128], P('gx', 'gy', 'gz'), may hold values from 0.5 to 2
- cell_matrix: float32 [81, 81], replicated, may hold values from -2 to 16, as said below
- face_coupling: float32 [3, 81, 81], replicated, may hold values from -0.18 to 0.18
- patch_inverse: bfloat16 [648, 648], replicated, may hold values from -0.01 to 0.1, as said below
Outputs:
- solution: float32 [81, 16, 16, 512], P(None, 'gx', 'gy', 'gz')
- residual: float32 [81, 16, 16, 512], P(None, 'gx', 'gy', 'gz')
The draws below stay inside these ranges and needn't reach their ends.
Inputs may be any that keep to these rules, and one draw needn't show every extreme that they name: `cell_matrix`: symmetric. `patch_inverse`: symmetric.
All inputs are finite; a program needn't handle non-finite values.
Results may differ from the reference program's by a relative error of at most 0.035.
Values may be sent and summed in bfloat16 or wider, within the bound.
A program may use at most 192 MiB of HBM per device.

```python
import math
import jax
import jax.numpy as jnp
from jax import lax

Q = 81
PATCH = 648
RHS = 4
NX = 16
NY = 16
NZ = 128


def symmetric_part(key, matrix_order):
    sampled = jnp.clip(jax.random.normal(key, (matrix_order, matrix_order), jnp.float32), -4.0, 4.0)
    return (sampled + sampled.T) * 0.7071


def draw_cell_matrix(key, part):
    key_diag = jax.random.fold_in(key, 11)
    key_rest = jax.random.fold_in(key, 12)
    diagonal = jax.random.uniform(key_diag, (Q,), jnp.float32, 10.8, 13.2)
    return jnp.diag(diagonal) + 0.35 * symmetric_part(key_rest, Q)


def draw_patch_inverse(key, part):
    key_diag = jax.random.fold_in(key, 21)
    key_rest = jax.random.fold_in(key, 22)
    diagonal = jax.random.uniform(key_diag, (PATCH,), jnp.float32, 0.9, 1.1)
    values = (jnp.diag(diagonal) + 0.012 * symmetric_part(key_rest, PATCH)) / 12.0
    return values.astype(jnp.bfloat16)


def shard_levels(stream_key, extent, split, low, largest):
    gain, own = 1.0, jax.random.fold_in(stream_key, 6)
    for position, parts in split:
        draws = jnp.exp(jax.random.uniform(jax.random.fold_in(own, position), (parts,), jnp.float32, low / len(split), largest / len(split)))
        gain = gain * jnp.repeat(draws, extent[position] // parts).reshape([-1 if axis == position else 1 for axis in range(len(extent))])
    return gain


def normal_values(key, dims, scale, limit, cuts=(), dtype=jnp.bfloat16):
    values = scale * jax.random.normal(key, dims, jnp.float32)
    if cuts:
        values = values * shard_levels(key, dims, cuts, -0.22, 0.18)
    return jnp.clip(values, -limit, limit).astype(dtype)


def setup_inputs(seed: int = 0) -> dict:
    keys = jax.random.split(jax.random.key(seed), 6)
    return {
        "right_side": normal_values(keys[0], (Q, NX, NY, NZ * RHS), 3.0, 18.0, ((1, 4), (2, 2), (3, 4)), jnp.float32),
        "cell_coef": jnp.clip(jnp.exp(math.log(2.0) - 1.3862944 * jax.random.uniform(keys[1], (NX, NY, NZ), jnp.float32) ** shard_levels(keys[1], (NX, NY, NZ), ((0, 4), (1, 2), (2, 4)), -0.2, 0.2)), 0.5, 2.0),
        "cell_matrix": draw_cell_matrix(jax.random.fold_in(keys[5], 71), 0),
        "face_coupling": normal_values(keys[3], (3, Q, Q), 0.03, 0.18, (), jnp.float32),
        "patch_inverse": draw_patch_inverse(jax.random.fold_in(keys[5], 71), 0),
    }


HIGH = lax.Precision.HIGHEST

def operator(values, cell_coef, cell_matrix, face_coupling):
    result = cell_coef[None, :, :, :, None] * jnp.einsum('pq,qxyzr->pxyzr', cell_matrix, values, precision=HIGH)
    for direction in range(3):
        forward = jnp.roll(values, -1, direction + 1)
        behind = jnp.roll(values, 1, direction + 1)
        result = result - jnp.einsum('pq,qxyzr->pxyzr', face_coupling[direction], forward, precision=HIGH)
        result = result - jnp.einsum('qp,qxyzr->pxyzr', face_coupling[direction], behind, precision=HIGH)
    return result

def reference(right_side, cell_coef, cell_matrix, face_coupling, patch_inverse):
    dof_count = cell_matrix.shape[0]
    residual = right_side.reshape(dof_count, NX, NY, NZ, RHS)
    solution = jnp.zeros_like(residual)
    scaling = lax.rsqrt(cell_coef)[None, :, :, :, None]
    blocks = patch_inverse.astype(jnp.float32).reshape(dof_count, 2, 2, 2, dof_count, 2, 2, 2)
    for colour in range(8):
        shifts = (1 - colour // 4, 1 - colour // 2 % 2, 1 - colour % 2)
        scaled = (scaling * residual).astype(jnp.bfloat16)
        scaled = lax.optimization_barrier(scaled).astype(jnp.float32)
        rolled = jnp.roll(scaled, shifts, axis=(1, 2, 3))
        blocked = rolled.reshape(dof_count, NX // 2, 2, NY // 2, 2, NZ // 2, 2, RHS)
        solved = jnp.einsum('qijkplmn,pXlYmZnr->qXiYjZkr', blocks, blocked, precision=HIGH)
        solved = solved.reshape(dof_count, NX, NY, NZ, RHS)
        solved = jnp.roll(solved, (-shifts[0], -shifts[1], -shifts[2]), axis=(1, 2, 3))
        correction = scaling * solved
        solution = solution + correction
        residual = residual - operator(correction, cell_coef, cell_matrix, face_coupling)
    return (solution.reshape(right_side.shape), residual.reshape(right_side.shape))
```

```python
import functools
import jax
import jax.numpy as jnp
from jax import lax
from jax.experimental import pallas as pl
from jax.experimental.pallas import tpu as pltpu
from jax.sharding import PartitionSpec as P

AXES = ("gx", "gy", "gz")
MESH = pl.DeviceIdType.MESH
F32, BF16 = jnp.float32, jnp.bfloat16
LANES = 128


def class_pairs(d):
    bit = 4 >> d
    return [(c, c + bit) for c in range(8) if not c & bit]


def kernel(sizes, dims, start_ref, p_ref, w_ref, sol_ref, res_ref,
           R, S, scaled, corr, ccorr, Xx, Xy, Xz,
           fx, fy, fz, fys, fzs, mxr, mxs, myr, mys, mzr, mzs,
           mxr_s, mxs_s, myr_s, mys_s, mzr_s, mzs_s, send_sem, recv_sem):
    D, Q, nr, ni, njh = dims
    w = 2 * nr
    tiles = [(i, jh) for i in range(ni) for jh in range(njh)]
    C = ni * njh * LANES
    half = njh * LANES
    lane = lax.broadcasted_iota(jnp.int32, (D, LANES), 1)
    jlo0 = (lane // nr) % 2 == 0
    piece = lane // w

    me = [lax.axis_index(a) for a in AXES]

    def neighbour(d, step):
        n = sizes[d]
        return {AXES[d]: lax.rem(me[d] + step + n, n)}

    barrier = pltpu.get_barrier_semaphore()
    for d in range(3):
        for step in (1, -1):
            pl.semaphore_signal(barrier, inc=1, device_id=neighbour(d, step), device_id_type=MESH)

    def rows(c):
        return slice(c * D, (c + 1) * D)

    def cols(i, jh):
        t = i * njh + jh
        return slice(t * LANES, (t + 1) * LANES)

    def get(ref, c):
        return {t: ref[rows(c), cols(*t)].astype(F32) for t in tiles}

    def roll(x, s):
        s = s % LANES
        return pltpu.roll(x, s, 1) if s else x

    for c in range(0, 8, 2):
        ox, oy = c // 4, c // 2 % 2
        for i, jh in tiles:
            a = start_ref[2 * i + ox, 4 * jh + oy]
            b = start_ref[2 * i + ox, 4 * jh + 2 + oy]
            R[rows(c), cols(i, jh)] = jnp.where(jlo0, a, roll(b, nr))
            R[rows(c + 1), cols(i, jh)] = jnp.where(jlo0, roll(a, -nr), b)
    S[...] = jnp.zeros_like(S)
    pl.semaphore_wait(barrier, 6)

    def pack_x(ref, d, last):
        i = ni - 1 if last else 0
        return jnp.concatenate(
            [ref[rows(p[1] if last else p[0]), i * half:(i + 1) * half] for p in class_pairs(0)], 0)

    def pack_y(ref, last):
        out = []
        for p in class_pairs(1):
            c = p[1] if last else p[0]
            jh = njh - 1 if last else 0
            t0 = ref[rows(c), cols(0, jh)].astype(F32)
            t1 = ref[rows(c), cols(1, jh)].astype(F32)
            if last:
                out.append(jnp.where(jlo0, roll(t1, -nr), t0))
            else:
                out.append(jnp.where(jlo0, t0, roll(t1, nr)))
        return jnp.concatenate(out, 0)

    def pack_z(ref, last):
        acc = jnp.zeros((D, LANES), F32)
        n = 0
        for p in class_pairs(2):
            c = p[1] if last else p[0]
            for t in tiles:
                x = ref[rows(c), cols(*t)].astype(F32)
                x = roll(x, w * (n + 1) if last else w * n)
                acc = jnp.where(piece == n, x, acc)
                n += 1
        return acc

    def shifted(d, step, have, halo, pc):
        out = {}
        for i, jh in tiles:
            if d == 0:
                at = i + step
                if 0 <= at < ni:
                    new = have[at, jh]
                else:
                    new = halo(rows(pc), slice(jh * LANES, (jh + 1) * LANES))
            elif d == 1:
                at = jh + step
                if 0 <= at < njh:
                    other = roll(have[i, at], step * nr)
                else:
                    other = halo(rows(pc), slice(0, LANES))
                    if i == 0:
                        other = roll(other, step * nr)
                cur = roll(have[i, jh], -step * nr)
                new = jnp.where(jlo0, cur, other) if step == 1 else jnp.where(jlo0, other, cur)
            else:
                n = pc * len(tiles) + i * njh + jh
                h = halo(slice(0, D), slice(0, LANES))
                if step == 1:
                    new = jnp.where(lane >= LANES - w, roll(h, LANES - w - w * n),
                                    roll(have[i, jh], -w))
                else:
                    new = jnp.where(lane < w, roll(h, -w * n), roll(have[i, jh], w))
            out[i, jh] = new
        return out

    def reader(ref, *at):
        return lambda r, c: ref[(*at, r, c)].astype(F32)

    def remote(src, dst, k, d, step):
        return pltpu.make_async_remote_copy(
            src_ref=src, dst_ref=dst, send_sem=send_sem.at[k], recv_sem=recv_sem.at[k],
            device_id=neighbour(d, step), device_id_type=MESH)

    packers = (lambda ref, last: pack_x(ref, 0, last), pack_y, pack_z)

    def move(d, down, items):
        step = 1 if down else -1
        copies = []
        for ref, staging, landing, at, k in items:
            staging[...] = packers[d](ref, down).astype(staging.dtype)
            copy = remote(staging, landing.at[at], k, d, step)
            copy.start()
            copies.append(copy)
        for (ref, staging, landing, at, k), copy in zip(items, copies):
            copy.wait()
            for pc, (c0, c1) in enumerate(class_pairs(d)):
                old0, old1 = get(ref, c0), get(ref, c1)
                if down:
                    new0, new1 = shifted(d, -1, old1, reader(landing, at), pc), old0
                else:
                    new0, new1 = old1, shifted(d, 1, old0, reader(landing, at), pc)
                for t in tiles:
                    ref[rows(c0), cols(*t)] = new0[t]
                    ref[rows(c1), cols(*t)] = new1[t]

    def pair_rows(q):
        return slice(2 * q * D, 2 * (q + 1) * D)

    def dot(a, b):
        return jnp.dot(a, b, preferred_element_type=F32)

    def colour(t):
        for c in range(8):
            s = R[c * D + Q:c * D + Q + 1, :]
            scaled[rows(c), :] = (s * R[rows(c), :]).astype(BF16)
        for n in range(ni):
            part = slice(n * half, (n + 1) * half)
            solved = dot(p_ref[...], scaled[:, part])
            for c in range(8):
                s = R[c * D + Q:c * D + Q + 1, part]
                k = R[c * D + Q + 1:c * D + Q + 2, part]
                got = s * solved[rows(c), :]
                S[rows(c), part] += got
                corr[rows(c), part] = got.astype(BF16)
                ccorr[rows(c), part] = (k * got).astype(BF16)
        copies = [[None, None] for _ in range(3)]
        for last in (0, 1):
            src = corr.at[4 * D:, half * (ni - 1):] if last else corr.at[:4 * D, :half]
            copies[0][last] = remote(src, fx.at[t, last], t * 6 + last, 0, 1 if last else -1)
            copies[0][last].start()
        for last in (0, 1):
            fys[last] = pack_y(corr, last).astype(BF16)
            copies[1][last] = remote(fys.at[last], fy.at[t, last], t * 6 + 2 + last, 1, 1 if last else -1)
            copies[1][last].start()
        for last in (0, 1):
            fzs[last] = pack_z(corr, last).astype(BF16)
            copies[2][last] = remote(fzs.at[last], fz.at[t, last], t * 6 + 4 + last, 2, 1 if last else -1)
            copies[2][last].start()
        for q in range(4):
            acc = dot(w_ref[0], ccorr[pair_rows(q), :])
            acc += dot(w_ref[1], corr[pair_rows(q), :])
            acc += dot(w_ref[3 if q // 2 == 0 else 4], corr[pair_rows(q ^ 2), :])
            acc += dot(w_ref[5 if q % 2 == 0 else 6], corr[pair_rows(q ^ 1), :])
            R[pair_rows(q), :] -= acc
        for d, X, landing in ((2, Xz, fz), (1, Xy, fy), (0, Xx, fx)):
            for copy in copies[d]:
                copy.wait()
            for pc, (c0, c1) in enumerate(class_pairs(d)):
                new0 = shifted(d, 1, get(corr, c0), reader(landing, t, 0), pc)
                new1 = shifted(d, -1, get(corr, c1), reader(landing, t, 1), pc)
                for at in tiles:
                    X[rows(c0), cols(*at)] = new0[at].astype(BF16)
                    X[rows(c1), cols(*at)] = new1[at].astype(BF16)
        for q in range(4):
            acc = dot(w_ref[2], Xz[pair_rows(q), :])
            acc += dot(w_ref[4 if q // 2 == 0 else 3], Xx[pair_rows(q ^ 2), :])
            acc += dot(w_ref[6 if q % 2 == 0 else 5], Xy[pair_rows(q ^ 1), :])
            R[pair_rows(q), :] -= acc

    def body(u, carry):
        @pl.when(u == 0)
        def _():
            move(0, True, [(R, mxr_s, mxr, 0, 72)])

        @pl.when(u == 2)
        def _():
            move(0, False, [(R, mxr_s, mxr, 1, 73), (S, mxs_s, mxs, 0, 74)])

        @pl.when(lax.rem(u, 2) == 0)
        def _():
            move(1, True, [(R, myr_s, myr, u, 64 + u), (S, mys_s, mys, u, 68 + u)])

        @pl.when(lax.rem(u, 2) == 1)
        def _():
            move(1, False, [(R, myr_s, myr, u, 64 + u), (S, mys_s, mys, u, 68 + u)])

        for v in (0, 1):
            t = 2 * u + v
            move(2, v == 0, [(R, mzr_s, mzr, t, 48 + t), (S, mzs_s, mzs, t, 56 + t)])
            colour(t)
        return carry

    lax.fori_loop(0, 4, body, 0)

    for ref, out in ((S, sol_ref), (R, res_ref)):
        for c in range(0, 8, 2):
            ox, oy = c // 4, c // 2 % 2
            for i, jh in tiles:
                x0 = ref[rows(c), cols(i, jh)]
                x1 = ref[rows(c + 1), cols(i, jh)]
                out[2 * i + ox, 4 * jh + oy] = jnp.where(jlo0, x0, roll(x1, nr))
                out[2 * i + ox, 4 * jh + 2 + oy] = jnp.where(jlo0, roll(x0, -nr), x1)


def on_device(sizes, right_side, cell_coef, cell_matrix, face_coupling, patch_inverse):
    Q = cell_matrix.shape[0]
    X, Y, Z = cell_coef.shape
    lanes = right_side.shape[3]
    nr = lanes // Z
    D = -(-(Q + 2) // 16) * 16
    ni, njh = X // 2, Y // 4
    assert lanes == LANES and ni == 2 and 4 * ni * njh * 2 * nr == LANES
    C = ni * njh * LANES
    coef = jnp.repeat(cell_coef, nr, axis=2)
    extra = jnp.stack([lax.rsqrt(coef), coef], 2)
    start = jnp.concatenate(
        [jnp.transpose(right_side, (1, 2, 0, 3)), extra, jnp.zeros((X, Y, D - Q - 2, lanes), F32)], 2)
    at = jnp.arange(8 * D)
    wanted = jnp.where(at % D < Q, at % D * 8 + at // D, -1)
    pick = (wanted[:, None] == jnp.arange(8 * Q)[None, :]).astype(BF16)
    p = jnp.dot(pick, patch_inverse, preferred_element_type=F32).astype(BF16)
    p = lax.dot_general(p, pick, (((1,), (1,)), ((), ())), preferred_element_type=F32).astype(BF16)

    def padded(m):
        return jnp.pad(m, ((0, D - Q), (0, D - Q)))

    zero = jnp.zeros((D, D), F32)

    def both(a, b, c, d):
        return jnp.concatenate([jnp.concatenate([a, b], 1), jnp.concatenate([c, d], 1)], 0)

    m = padded(cell_matrix)
    f = [-padded(face_coupling[d]) for d in range(3)]
    ft = [x.T for x in f]
    mats = jnp.stack([
        both(m, zero, zero, m),
        both(zero, f[2], ft[2], zero),
        both(zero, ft[2], f[2], zero),
        both(f[0], zero, zero, f[0]),
        both(ft[0], zero, zero, ft[0]),
        both(f[1], zero, zero, f[1]),
        both(ft[1], zero, zero, ft[1]),
    ]).astype(BF16)
    half = njh * LANES
    V = pltpu.VMEM
    scratch = [
        V((8 * D, C), F32), V((8 * D, C), F32), V((8 * D, C), BF16), V((8 * D, C), BF16),
        V((8 * D, C), BF16), V((8 * D, C), BF16), V((8 * D, C), BF16), V((8 * D, C), BF16),
        V((8, 2, 4 * D, half), BF16), V((8, 2, 4 * D, LANES), BF16), V((8, 2, D, LANES), BF16),
        V((2, 4 * D, LANES), BF16), V((2, D, LANES), BF16),
        V((2, 4 * D, half), F32), V((1, 4 * D, half), BF16),
        V((4, 4 * D, LANES), F32), V((4, 4 * D, LANES), BF16),
        V((8, D, LANES), F32), V((8, D, LANES), BF16),
        V((4 * D, half), F32), V((4 * D, half), BF16),
        V((4 * D, LANES), F32), V((4 * D, LANES), BF16),
        V((D, LANES), F32), V((D, LANES), BF16),
        pltpu.SemaphoreType.DMA((75,)), pltpu.SemaphoreType.DMA((75,)),
    ]
    vmem = pl.BlockSpec(memory_space=pltpu.VMEM)
    sol, res = pl.pallas_call(
        functools.partial(kernel, sizes, (D, Q, nr, ni, njh)),
        out_shape=[jax.ShapeDtypeStruct((X, Y, D, lanes), F32)] * 2,
        in_specs=[vmem] * 3,
        out_specs=[vmem] * 2,
        scratch_shapes=scratch,
        compiler_params=pltpu.CompilerParams(
            collective_id=0, has_side_effects=True, vmem_limit_bytes=60 * 1024 * 1024),
    )(start, p, mats)
    return tuple(jnp.transpose(x[:, :, :Q], (2, 0, 1, 3)) for x in (sol, res))


def solution(mesh):
    sizes = tuple(mesh.shape[a] for a in AXES)
    placed = (P(None, "gx", "gy", "gz"), P("gx", "gy", "gz"), P(), P(), P())
    return jax.shard_map(
        functools.partial(on_device, sizes),
        mesh=mesh,
        in_specs=placed,
        out_specs=(P(None, "gx", "gy", "gz"), P(None, "gx", "gy", "gz")),
        check_vma=False,
    )
```

```python
import functools
import jax
import jax.numpy as jnp
from jax import lax
from jax.experimental import pallas as pl
from jax.experimental.pallas import tpu as pltpu
from jax.sharding import PartitionSpec as P

AXES = ("gx", "gy", "gz")
MESH = pl.DeviceIdType.MESH
F32, BF16 = jnp.float32, jnp.bfloat16
LANES = 128


def class_pairs(d):
    bit = 4 >> d
    return [(c, c + bit) for c in range(8) if not c & bit]


def kernel(sizes, dims, start_ref, p_ref, w_ref, sol_ref, res_ref,
           R, S2, Sx, scaled, corr, ccorr, Xx, Xy, Xz,
           fx, fxe, fy, fz, fxes, fys, fzs, mxr, mxe, mxs, myr, mys, mzr,
           mxr_s, mxs_s, myr_s, mys_s, mzr_s, send_sem, recv_sem):
    D, Q, nr, ni, njh = dims
    w = 2 * nr
    A = Q // 16 * 16
    tiles = [(i, jh) for i in range(ni) for jh in range(njh)]
    C = ni * njh * LANES
    half = njh * LANES
    lane = lax.broadcasted_iota(jnp.int32, (D, LANES), 1)
    jlo0 = (lane // nr) % 2 == 0
    piece = lane // w

    me = [lax.axis_index(a) for a in AXES]

    def neighbour(d, step):
        n = sizes[d]
        return {AXES[d]: lax.rem(me[d] + step + n, n)}

    barrier = pltpu.get_barrier_semaphore()
    for d in range(3):
        for step in (1, -1):
            pl.semaphore_signal(barrier, inc=1, device_id=neighbour(d, step), device_id_type=MESH)

    def rows(c):
        return slice(c * D, (c + 1) * D)

    def cols(i, jh):
        t = i * njh + jh
        return slice(t * LANES, (t + 1) * LANES)

    def get(ref, c):
        return {t: ref[c, :, cols(*t)].astype(F32) for t in tiles}

    def roll(x, s):
        s = s % LANES
        return pltpu.roll(x, s, 1) if s else x

    for c in range(0, 8, 2):
        ox, oy = c // 4, c // 2 % 2
        for i, jh in tiles:
            a = start_ref[2 * i + ox, 4 * jh + oy]
            b = start_ref[2 * i + ox, 4 * jh + 2 + oy]
            R[c, :, cols(i, jh)] = jnp.where(jlo0, a, roll(b, nr))
            R[c + 1, :, cols(i, jh)] = jnp.where(jlo0, roll(a, -nr), b)
    S2[...] = jnp.zeros_like(S2)
    pl.semaphore_wait(barrier, 6)

    def pack_y(ref, last):
        out = []
        for p in class_pairs(1):
            c = p[1] if last else p[0]
            jh = njh - 1 if last else 0
            t0 = ref[c, :, cols(0, jh)].astype(F32)
            t1 = ref[c, :, cols(1, jh)].astype(F32)
            if last:
                out.append(jnp.where(jlo0, roll(t1, -nr), t0))
            else:
                out.append(jnp.where(jlo0, t0, roll(t1, nr)))
        return jnp.stack(out, 0)

    def pack_z(ref, last):
        acc = jnp.zeros((D, LANES), F32)
        n = 0
        for p in class_pairs(2):
            c = p[1] if last else p[0]
            for t in tiles:
                x = ref[c, :, cols(*t)].astype(F32)
                x = roll(x, w * (n + 1) if last else w * n)
                acc = jnp.where(piece == n, x, acc)
                n += 1
        return acc

    def shifted(d, step, have, halo, pc):
        out = {}
        for i, jh in tiles:
            if d == 0:
                at = i + step
                if 0 <= at < ni:
                    new = have[at, jh]
                else:
                    new = halo(slice(jh * LANES, (jh + 1) * LANES))
            elif d == 1:
                at = jh + step
                if 0 <= at < njh:
                    other = roll(have[i, at], step * nr)
                else:
                    other = halo(slice(0, LANES))
                    if i == 0:
                        other = roll(other, step * nr)
                cur = roll(have[i, jh], -step * nr)
                new = jnp.where(jlo0, cur, other) if step == 1 else jnp.where(jlo0, other, cur)
            else:
                n = pc * len(tiles) + i * njh + jh
                h = halo(slice(0, LANES))
                if step == 1:
                    new = jnp.where(lane >= LANES - w, roll(h, LANES - w - w * n),
                                    roll(have[i, jh], -w))
                else:
                    new = jnp.where(lane < w, roll(h, -w * n), roll(have[i, jh], w))
            out[i, jh] = new
        return out

    def read_x(t, last, pc):
        first = lax.broadcasted_iota(jnp.int32, (D - A, LANES), 0) == 0

        def halo(c):
            tail = fxe[t, last, :, c].astype(F32)[pc:pc + 1]
            return jnp.concatenate(
                [fx[t, last, pc, :, c].astype(F32), jnp.where(first, tail, 0.0)], 0)
        return halo

    def read_y(ref, *at):
        return lambda c: ref[(*at, slice(None), c)].astype(F32)

    def remote(src, dst, k, d, step):
        return pltpu.make_async_remote_copy(
            src_ref=src, dst_ref=dst, send_sem=send_sem.at[k], recv_sem=recv_sem.at[k],
            device_id=neighbour(d, step), device_id_type=MESH)

    def move(d, down, copies, halo):
        for copy in copies:
            copy.start()
        for copy in copies:
            copy.wait()
        for pc, (c0, c1) in enumerate(class_pairs(d)):
            old0, old1 = get(R, c0), get(R, c1)
            if down:
                new0, new1 = shifted(d, -1, old1, halo(pc), pc), old0
            else:
                new0, new1 = old1, shifted(d, 1, old0, halo(pc), pc)
            for t in tiles:
                R[c0, :, cols(*t)] = new0[t]
                R[c1, :, cols(*t)] = new1[t]

    def move_x(down, at):
        part = slice((ni - 1) * half, ni * half) if down else slice(0, half)
        cs = slice(4, 8) if down else slice(0, 4)
        mxr_s[...] = R[cs, :A, part].astype(BF16)
        step = 1 if down else -1
        copies = [remote(mxr_s, mxr.at[at], 72 + at, 0, step),
                  remote(R.at[cs, A:A + 8, part], mxe.at[at], 74 + at, 0, step)]
        zeros = jnp.zeros((D - A - 8, LANES), F32)

        def halo(pc):
            return lambda c: jnp.concatenate(
                [mxr[at, pc, :, c].astype(F32), mxe[at, pc, :, c], zeros], 0)
        move(0, down, copies, halo)

    def move_y(down, u):
        myr_s[...] = pack_y(R, down)
        move(1, down, [remote(myr_s, myr.at[u], 64 + u, 1, 1 if down else -1)],
             lambda pc: read_y(myr, u, pc))

    def move_z(down, t):
        mzr_s[...] = pack_z(R, down)
        move(2, down, [remote(mzr_s, mzr.at[t], 48 + t, 2, 1 if down else -1)],
             lambda pc: read_y(mzr, t))

    def sol_y(u):
        return remote(mys_s, mys.at[lax.div(u, 2)], 56 + lax.div(u, 2), 1, -1)

    def sol_x():
        return remote(mxs_s, mxs, 58, 0, -1)

    def pair(ref, q):
        return ref[2 * q:2 * q + 2].reshape(2 * D, C)

    def lessen(q, acc):
        R[2 * q:2 * q + 2] -= acc.reshape(2, D, C)

    def dot(a, b):
        return jnp.dot(a, b, preferred_element_type=F32)

    def colour(t, v, sb):
        for c in range(8):
            s = R[c, Q:Q + 1, :]
            scaled[c] = (s * R[c]).astype(BF16)
        copies = [[None, None] for _ in range(3)]
        extra = [None, None]
        line = lax.broadcasted_iota(jnp.int32, (16, half), 0)
        for n in range(ni):
            part = slice(n * half, (n + 1) * half)
            solved = dot(p_ref[...], scaled[:, :, part].reshape(8 * D, half))
            for c in range(8):
                s = R[c, Q:Q + 1, part]
                k = R[c, Q + 1:Q + 2, part]
                got = s * solved[rows(c), :]
                if v == 1:
                    S2[sb, c, :, part] += got
                corr[c, :, part] = got.astype(BF16)
                ccorr[c, :, part] = (k * got).astype(BF16)
            for last in (0, 1):
                if n != (ni - 1 if last else 0):
                    continue
                step = 1 if last else -1
                tail = jnp.zeros((16, half), F32)
                for pc in range(4):
                    row = corr[4 * last + pc, A:, part].astype(F32)[:1]
                    tail = jnp.where(line == pc, row, tail)
                fxes[last] = tail.astype(BF16)
                copies[0][last] = remote(corr.at[4 * last:4 * last + 4, :A, part], fx.at[t, last],
                                         t * 6 + last, 0, step)
                copies[0][last].start()
                extra[last] = remote(fxes.at[last], fxe.at[t, last], 80 + 2 * t + last, 0, step)
                extra[last].start()
        for last in (0, 1):
            fzs[last] = pack_z(corr, last).astype(BF16)
            copies[2][last] = remote(fzs.at[last], fz.at[t, last], t * 6 + 4 + last, 2, 1 if last else -1)
            copies[2][last].start()
        for last in (0, 1):
            fys[last] = pack_y(corr, last).astype(BF16)
            copies[1][last] = remote(fys.at[last], fy.at[t, last], t * 6 + 2 + last, 1, 1 if last else -1)
            copies[1][last].start()
        for q in range(4):
            acc = dot(w_ref[0], pair(ccorr, q))
            acc += dot(w_ref[1], pair(corr, q))
            acc += dot(w_ref[3 if q // 2 == 0 else 4], pair(corr, q ^ 2))
            acc += dot(w_ref[5 if q % 2 == 0 else 6], pair(corr, q ^ 1))
            lessen(q, acc)

        def fill(d, X, halo0, halo1):
            for pc, (c0, c1) in enumerate(class_pairs(d)):
                new0 = shifted(d, 1, get(corr, c0), halo0(pc), pc)
                new1 = shifted(d, -1, get(corr, c1), halo1(pc), pc)
                for at in tiles:
                    X[c0, :, cols(*at)] = new0[at].astype(BF16)
                    X[c1, :, cols(*at)] = new1[at].astype(BF16)

        for copy in copies[2]:
            copy.wait()
        fill(2, Xz, lambda pc: read_y(fz, t, 0), lambda pc: read_y(fz, t, 1))
        if v == 0:
            for c0, c1 in class_pairs(2):
                S2[sb, c0] += corr[c1].astype(F32)
                S2[sb, c1] += Xz[c0].astype(F32)
        for copy in copies[1]:
            copy.wait()
        fill(1, Xy, lambda pc: read_y(fy, t, 0, pc), lambda pc: read_y(fy, t, 1, pc))
        for q in range(4):
            acc = dot(w_ref[2], pair(Xz, q))
            acc += dot(w_ref[6 if q % 2 == 0 else 5], pair(Xy, q ^ 1))
            lessen(q, acc)
        for copy in copies[0] + extra:
            copy.wait()
        fill(0, Xx, lambda pc: read_x(t, 0, pc), lambda pc: read_x(t, 1, pc))
        for q in range(4):
            lessen(q, dot(w_ref[4 if q // 2 == 0 else 3], pair(Xx, q ^ 2)))

    def body(u, carry):
        @pl.when(u == 0)
        def _():
            move_x(True, 0)

        @pl.when(u == 2)
        def _():
            move_x(False, 1)
            for c in range(8):
                Sx[c] = S2[1, c]
            mxs_s[...] = S2[1, :4, :, :half].astype(BF16)
            sol_x().start()
            S2[1] = jnp.zeros_like(Sx)

        @pl.when(lax.rem(u, 2) == 0)
        def _():
            S2[0] = jnp.zeros_like(Sx)
            move_y(True, u)

        @pl.when(lax.rem(u, 2) == 1)
        def _():
            move_y(False, u)
            mys_s[...] = pack_y(S2.at[0], False).astype(BF16)
            sol_y(u).start()

        for v in (0, 1):
            t = 2 * u + v
            move_z(v == 0, t)
            colour(t, v, lax.rem(u, 2))

        @pl.when(lax.rem(u, 2) == 1)
        def _():
            sol_y(u).wait()
            for pc, (c0, c1) in enumerate(class_pairs(1)):
                S2[1, c0] += S2[0, c1]
                new = shifted(1, 1, get(S2.at[0], c0), read_y(mys, lax.div(u, 2), pc), pc)
                for at in tiles:
                    S2[1, c1, :, cols(*at)] += new[at]
        return carry

    lax.fori_loop(0, 4, body, 0)
    sol_x().wait()
    for pc, (c0, c1) in enumerate(class_pairs(0)):
        S2[1, c0] += Sx[c1]
        new = shifted(0, 1, get(Sx, c0), read_y(mxs, pc), pc)
        for at in tiles:
            S2[1, c1, :, cols(*at)] += new[at]

    for ref, out in ((S2.at[1], sol_ref), (R, res_ref)):
        for c in range(0, 8, 2):
            ox, oy = c // 4, c // 2 % 2
            for i, jh in tiles:
                x0 = ref[c, :, cols(i, jh)]
                x1 = ref[c + 1, :, cols(i, jh)]
                out[2 * i + ox, 4 * jh + oy] = jnp.where(jlo0, x0, roll(x1, nr))
                out[2 * i + ox, 4 * jh + 2 + oy] = jnp.where(jlo0, roll(x0, -nr), x1)


def on_device(sizes, right_side, cell_coef, cell_matrix, face_coupling, patch_inverse):
    Q = cell_matrix.shape[0]
    X, Y, Z = cell_coef.shape
    lanes = right_side.shape[3]
    nr = lanes // Z
    D = -(-(Q + 2) // 16) * 16
    ni, njh = X // 2, Y // 4
    assert lanes == LANES and ni == 2 and 4 * ni * njh * 2 * nr == LANES
    C = ni * njh * LANES
    coef = jnp.repeat(cell_coef, nr, axis=2)
    extra = jnp.stack([lax.rsqrt(coef), coef], 2)
    start = jnp.concatenate(
        [jnp.transpose(right_side, (1, 2, 0, 3)), extra, jnp.zeros((X, Y, D - Q - 2, lanes), F32)], 2)
    at = jnp.arange(8 * D)
    wanted = jnp.where(at % D < Q, at % D * 8 + at // D, -1)
    pick = (wanted[:, None] == jnp.arange(8 * Q)[None, :]).astype(BF16)
    p = jnp.dot(pick, patch_inverse, preferred_element_type=F32).astype(BF16)
    p = lax.dot_general(p, pick, (((1,), (1,)), ((), ())), preferred_element_type=F32).astype(BF16)

    def padded(m):
        return jnp.pad(m, ((0, D - Q), (0, D - Q)))

    zero = jnp.zeros((D, D), F32)

    def both(a, b, c, d):
        return jnp.concatenate([jnp.concatenate([a, b], 1), jnp.concatenate([c, d], 1)], 0)

    m = padded(cell_matrix)
    f = [-padded(face_coupling[d]) for d in range(3)]
    ft = [x.T for x in f]
    mats = jnp.stack([
        both(m, zero, zero, m),
        both(zero, f[2], ft[2], zero),
        both(zero, ft[2], f[2], zero),
        both(f[0], zero, zero, f[0]),
        both(ft[0], zero, zero, ft[0]),
        both(f[1], zero, zero, f[1]),
        both(ft[1], zero, zero, ft[1]),
    ]).astype(BF16)
    half = njh * LANES
    V = pltpu.VMEM
    A = Q // 16 * 16
    assert Q == A + 1
    whole = (8, D, C)
    scratch = [
        V(whole, F32), V((2, *whole), F32), V(whole, F32), V(whole, BF16), V(whole, BF16), V(whole, BF16),
        V(whole, BF16), V(whole, BF16), V(whole, BF16),
        V((8, 2, 4, A, half), BF16), V((8, 2, 16, half), BF16),
        V((8, 2, 4, D, LANES), BF16), V((8, 2, D, LANES), BF16),
        V((2, 16, half), BF16), V((2, 4, D, LANES), BF16), V((2, D, LANES), BF16),
        V((2, 4, A, half), BF16), V((2, 4, 8, half), F32), V((4, D, half), BF16),
        V((4, 4, D, LANES), F32), V((2, 4, D, LANES), BF16), V((8, D, LANES), F32),
        V((4, A, half), BF16), V((4, D, half), BF16),
        V((4, D, LANES), F32), V((4, D, LANES), BF16), V((D, LANES), F32),
        pltpu.SemaphoreType.DMA((96,)), pltpu.SemaphoreType.DMA((96,)),
    ]
    vmem = pl.BlockSpec(memory_space=pltpu.VMEM)
    sol, res = pl.pallas_call(
        functools.partial(kernel, sizes, (D, Q, nr, ni, njh)),
        out_shape=[jax.ShapeDtypeStruct((X, Y, D, lanes), F32)] * 2,
        in_specs=[vmem] * 3,
        out_specs=[vmem] * 2,
        scratch_shapes=scratch,
        compiler_params=pltpu.CompilerParams(
            collective_id=0, has_side_effects=True, vmem_limit_bytes=60 * 1024 * 1024),
    )(start, p, mats)
    return tuple(jnp.transpose(x[:, :, :Q], (2, 0, 1, 3)) for x in (sol, res))


def solution(mesh):
    sizes = tuple(mesh.shape[a] for a in AXES)
    placed = (P(None, "gx", "gy", "gz"), P("gx", "gy", "gz"), P(), P(), P())
    return jax.shard_map(
        functools.partial(on_device, sizes),
        mesh=mesh,
        in_specs=placed,
        out_specs=(P(None, "gx", "gy", "gz"), P(None, "gx", "gy", "gz")),
        check_vma=False,
    )
```

```python
import functools
import jax
import jax.numpy as jnp
from jax import lax
from jax.experimental import pallas as pl
from jax.experimental.pallas import tpu as pltpu
from jax.sharding import PartitionSpec as P

AXES = ("gx", "gy", "gz")
MESH = pl.DeviceIdType.MESH
F32, BF16 = jnp.float32, jnp.bfloat16
LANES = 128


def class_pairs(d):
    bit = 4 >> d
    return [(c, c + bit) for c in range(8) if not c & bit]


def kernel(sizes, dims, start_ref, inverse_ref, w_ref, sol_ref, res_ref,
           R, S2, Sx, scaled, corr, ccorr, Xx, Xy, Xz,
           fx, fxe, fy, fz, fxes, fys, fzs, mxr, mxe, mxs, myr, mys, mzr,
           mxr_s, mxs_s, myr_s, mys_s, mzr_s, p_rows, p_ref, send_sem, recv_sem):
    D, Q, nr, ni, njh = dims
    w = 2 * nr
    A = Q // 16 * 16
    tiles = [(i, jh) for i in range(ni) for jh in range(njh)]
    C = ni * njh * LANES
    half = njh * LANES
    lane = lax.broadcasted_iota(jnp.int32, (D, LANES), 1)
    jlo0 = (lane // nr) % 2 == 0
    piece = lane // w

    me = [lax.axis_index(a) for a in AXES]

    def neighbour(d, step):
        n = sizes[d]
        return {AXES[d]: lax.rem(me[d] + step + n, n)}

    barrier = pltpu.get_barrier_semaphore()
    for d in range(3):
        for step in (1, -1):
            pl.semaphore_signal(barrier, inc=1, device_id=neighbour(d, step), device_id_type=MESH)

    def rows(c):
        return slice(c * D, (c + 1) * D)

    def cols(i, jh):
        t = i * njh + jh
        return slice(t * LANES, (t + 1) * LANES)

    def get(ref, c):
        return {t: ref[c, :, cols(*t)].astype(F32) for t in tiles}

    def roll(x, s):
        s = s % LANES
        return pltpu.roll(x, s, 1) if s else x

    for c in range(0, 8, 2):
        ox, oy = c // 4, c // 2 % 2
        for i, jh in tiles:
            a = start_ref[2 * i + ox, 4 * jh + oy]
            b = start_ref[2 * i + ox, 4 * jh + 2 + oy]
            R[c, :, cols(i, jh)] = jnp.where(jlo0, a, roll(b, nr))
            R[c + 1, :, cols(i, jh)] = jnp.where(jlo0, roll(a, -nr), b)
    S2[...] = jnp.zeros_like(S2)
    pl.semaphore_wait(barrier, 6)

    def pack_y(ref, last):
        out = []
        for p in class_pairs(1):
            c = p[1] if last else p[0]
            jh = njh - 1 if last else 0
            t0 = ref[c, :, cols(0, jh)].astype(F32)
            t1 = ref[c, :, cols(1, jh)].astype(F32)
            if last:
                out.append(jnp.where(jlo0, roll(t1, -nr), t0))
            else:
                out.append(jnp.where(jlo0, t0, roll(t1, nr)))
        return jnp.stack(out, 0)

    def pack_z(ref, last):
        acc = jnp.zeros((D, LANES), F32)
        n = 0
        for p in class_pairs(2):
            c = p[1] if last else p[0]
            for t in tiles:
                x = ref[c, :, cols(*t)].astype(F32)
                x = roll(x, w * (n + 1) if last else w * n)
                acc = jnp.where(piece == n, x, acc)
                n += 1
        return acc

    def shifted(d, step, have, halo, pc):
        out = {}
        for i, jh in tiles:
            if d == 0:
                at = i + step
                if 0 <= at < ni:
                    new = have[at, jh]
                else:
                    new = halo(slice(jh * LANES, (jh + 1) * LANES))
            elif d == 1:
                at = jh + step
                if 0 <= at < njh:
                    other = roll(have[i, at], step * nr)
                else:
                    other = halo(slice(0, LANES))
                    if i == 0:
                        other = roll(other, step * nr)
                cur = roll(have[i, jh], -step * nr)
                new = jnp.where(jlo0, cur, other) if step == 1 else jnp.where(jlo0, other, cur)
            else:
                n = pc * len(tiles) + i * njh + jh
                h = halo(slice(0, LANES))
                if step == 1:
                    new = jnp.where(lane >= LANES - w, roll(h, LANES - w - w * n),
                                    roll(have[i, jh], -w))
                else:
                    new = jnp.where(lane < w, roll(h, -w * n), roll(have[i, jh], w))
            out[i, jh] = new
        return out

    def read_x(t, last, pc):
        first = lax.broadcasted_iota(jnp.int32, (D - A, LANES), 0) == 0

        def halo(c):
            tail = fxe[t, last, :, c].astype(F32)[pc:pc + 1]
            return jnp.concatenate(
                [fx[t, last, pc, :, c].astype(F32), jnp.where(first, tail, 0.0)], 0)
        return halo

    def read_y(ref, *at):
        return lambda c: ref[(*at, slice(None), c)].astype(F32)

    def remote(src, dst, k, d, step):
        return pltpu.make_async_remote_copy(
            src_ref=src, dst_ref=dst, send_sem=send_sem.at[k], recv_sem=recv_sem.at[k],
            device_id=neighbour(d, step), device_id_type=MESH)

    def move(d, down, copies, halo, beside=None):
        for copy in copies:
            copy.start()
        if beside is not None:
            beside()
        for copy in copies:
            copy.wait()
        for pc, (c0, c1) in enumerate(class_pairs(d)):
            old0, old1 = get(R, c0), get(R, c1)
            if down:
                new0, new1 = shifted(d, -1, old1, halo(pc), pc), old0
            else:
                new0, new1 = old1, shifted(d, 1, old0, halo(pc), pc)
            for t in tiles:
                R[c0, :, cols(*t)] = new0[t]
                R[c1, :, cols(*t)] = new1[t]

    def move_x(down, at, beside=None):
        part = slice((ni - 1) * half, ni * half) if down else slice(0, half)
        cs = slice(4, 8) if down else slice(0, 4)
        mxr_s[...] = R[cs, :A, part].astype(BF16)
        step = 1 if down else -1
        copies = [remote(mxr_s, mxr.at[at], 72 + at, 0, step),
                  remote(R.at[cs, A:A + 8, part], mxe.at[at], 74 + at, 0, step)]
        zeros = jnp.zeros((D - A - 8, LANES), F32)

        def halo(pc):
            return lambda c: jnp.concatenate(
                [mxr[at, pc, :, c].astype(F32), mxe[at, pc, :, c], zeros], 0)
        move(0, down, copies, halo, beside)

    def move_y(down, u):
        myr_s[...] = pack_y(R, down)
        move(1, down, [remote(myr_s, myr.at[u], 64 + u, 1, 1 if down else -1)],
             lambda pc: read_y(myr, u, pc))

    def move_z(down, t):
        mzr_s[...] = pack_z(R, down)
        move(2, down, [remote(mzr_s, mzr.at[t], 48 + t, 2, 1 if down else -1)],
             lambda pc: read_y(mzr, t))

    def sol_y(u):
        return remote(mys_s, mys.at[lax.div(u, 2)], 56 + lax.div(u, 2), 1, -1)

    def sol_x():
        return remote(mxs_s, mxs, 58, 0, -1)

    def pair(ref, q):
        return ref[2 * q:2 * q + 2].reshape(2 * D, C)

    def lessen(q, acc):
        R[2 * q:2 * q + 2] -= acc.reshape(2, D, C)

    def dot(a, b):
        return jnp.dot(a, b, preferred_element_type=F32)

    def colour(t, v, sb):
        for c in range(8):
            s = R[c, Q:Q + 1, :]
            scaled[c] = (s * R[c]).astype(BF16)
        copies = [[None, None] for _ in range(3)]
        extra = [None, None]
        line = lax.broadcasted_iota(jnp.int32, (16, half), 0)
        for n in range(ni):
            part = slice(n * half, (n + 1) * half)
            solved = dot(p_ref[...], scaled[:, :, part].reshape(8 * D, half))
            for c in range(8):
                s = R[c, Q:Q + 1, part]
                k = R[c, Q + 1:Q + 2, part]
                got = s * solved[rows(c), :]
                if v == 1:
                    S2[sb, c, :, part] += got
                corr[c, :, part] = got.astype(BF16)
                ccorr[c, :, part] = (k * got).astype(BF16)
            for last in (0, 1):
                if n != (ni - 1 if last else 0):
                    continue
                step = 1 if last else -1
                tail = jnp.zeros((16, half), F32)
                for pc in range(4):
                    row = corr[4 * last + pc, A:, part].astype(F32)[:1]
                    tail = jnp.where(line == pc, row, tail)
                fxes[last] = tail.astype(BF16)
                copies[0][last] = remote(corr.at[4 * last:4 * last + 4, :A, part], fx.at[t, last],
                                         t * 6 + last, 0, step)
                copies[0][last].start()
                extra[last] = remote(fxes.at[last], fxe.at[t, last], 80 + 2 * t + last, 0, step)
                extra[last].start()
        for last in (0, 1):
            fzs[last] = pack_z(corr, last).astype(BF16)
            copies[2][last] = remote(fzs.at[last], fz.at[t, last], t * 6 + 4 + last, 2, 1 if last else -1)
            copies[2][last].start()
        for last in (0, 1):
            fys[last] = pack_y(corr, last).astype(BF16)
            copies[1][last] = remote(fys.at[last], fy.at[t, last], t * 6 + 2 + last, 1, 1 if last else -1)
            copies[1][last].start()
        for q in range(4):
            acc = dot(w_ref[0], pair(ccorr, q))
            acc += dot(w_ref[1], pair(corr, q))
            acc += dot(w_ref[3 if q // 2 == 0 else 4], pair(corr, q ^ 2))
            acc += dot(w_ref[5 if q % 2 == 0 else 6], pair(corr, q ^ 1))
            lessen(q, acc)

        def fill(d, X, halo0, halo1):
            for pc, (c0, c1) in enumerate(class_pairs(d)):
                new0 = shifted(d, 1, get(corr, c0), halo0(pc), pc)
                new1 = shifted(d, -1, get(corr, c1), halo1(pc), pc)
                for at in tiles:
                    X[c0, :, cols(*at)] = new0[at].astype(BF16)
                    X[c1, :, cols(*at)] = new1[at].astype(BF16)

        for copy in copies[2]:
            copy.wait()
        fill(2, Xz, lambda pc: read_y(fz, t, 0), lambda pc: read_y(fz, t, 1))
        if v == 0:
            for c0, c1 in class_pairs(2):
                S2[sb, c0] += corr[c1].astype(F32)
                S2[sb, c1] += Xz[c0].astype(F32)
        for copy in copies[1]:
            copy.wait()
        fill(1, Xy, lambda pc: read_y(fy, t, 0, pc), lambda pc: read_y(fy, t, 1, pc))
        for q in range(4):
            acc = dot(w_ref[2], pair(Xz, q))
            acc += dot(w_ref[6 if q % 2 == 0 else 5], pair(Xy, q ^ 1))
            lessen(q, acc)
        for copy in copies[0] + extra:
            copy.wait()
        fill(0, Xx, lambda pc: read_x(t, 0, pc), lambda pc: read_x(t, 1, pc))
        for q in range(4):
            lessen(q, dot(w_ref[4 if q // 2 == 0 else 3], pair(Xx, q ^ 2)))

    def class_order():
        r = lax.broadcasted_iota(jnp.int32, (D, 8 * Q), 0)
        k = lax.broadcasted_iota(jnp.int32, (D, 8 * Q), 1)
        for c in range(8):
            pick = jnp.where((k == r * 8 + c) & (r < Q), 1.0, 0.0).astype(BF16)
            p_rows[c * D:(c + 1) * D, :] = dot(pick, inverse_ref[...]).astype(BF16)
        k = lax.broadcasted_iota(jnp.int32, (8 * Q, 8 * D), 0)
        r = lax.broadcasted_iota(jnp.int32, (8 * Q, 8 * D), 1)
        q = r % D
        pick = jnp.where((k == q * 8 + r // D) & (q < Q), 1.0, 0.0).astype(BF16)
        p_ref[...] = dot(p_rows[...], pick).astype(BF16)

    def body(u, carry):
        @pl.when(u == 0)
        def _():
            move_x(True, 0, class_order)

        @pl.when(u == 2)
        def _():
            move_x(False, 1)
            for c in range(8):
                Sx[c] = S2[1, c]
            mxs_s[...] = S2[1, :4, :, :half].astype(BF16)
            sol_x().start()
            S2[1] = jnp.zeros_like(Sx)

        @pl.when(lax.rem(u, 2) == 0)
        def _():
            S2[0] = jnp.zeros_like(Sx)
            move_y(True, u)

        @pl.when(lax.rem(u, 2) == 1)
        def _():
            move_y(False, u)
            mys_s[...] = pack_y(S2.at[0], False).astype(BF16)
            sol_y(u).start()

        for v in (0, 1):
            t = 2 * u + v
            move_z(v == 0, t)
            colour(t, v, lax.rem(u, 2))

        @pl.when(lax.rem(u, 2) == 1)
        def _():
            sol_y(u).wait()
            for pc, (c0, c1) in enumerate(class_pairs(1)):
                S2[1, c0] += S2[0, c1]
                new = shifted(1, 1, get(S2.at[0], c0), read_y(mys, lax.div(u, 2), pc), pc)
                for at in tiles:
                    S2[1, c1, :, cols(*at)] += new[at]
        return carry

    lax.fori_loop(0, 4, body, 0)
    sol_x().wait()
    for pc, (c0, c1) in enumerate(class_pairs(0)):
        S2[1, c0] += Sx[c1]
        new = shifted(0, 1, get(Sx, c0), read_y(mxs, pc), pc)
        for at in tiles:
            S2[1, c1, :, cols(*at)] += new[at]

    for ref, out in ((S2.at[1], sol_ref), (R, res_ref)):
        for c in range(0, 8, 2):
            ox, oy = c // 4, c // 2 % 2
            for i, jh in tiles:
                x0 = ref[c, :, cols(i, jh)]
                x1 = ref[c + 1, :, cols(i, jh)]
                out[2 * i + ox, 4 * jh + oy] = jnp.where(jlo0, x0, roll(x1, nr))
                out[2 * i + ox, 4 * jh + 2 + oy] = jnp.where(jlo0, roll(x0, -nr), x1)


def on_device(sizes, right_side, cell_coef, cell_matrix, face_coupling, patch_inverse):
    Q = cell_matrix.shape[0]
    X, Y, Z = cell_coef.shape
    lanes = right_side.shape[3]
    nr = lanes // Z
    D = -(-(Q + 2) // 16) * 16
    ni, njh = X // 2, Y // 4
    assert lanes == LANES and ni == 2 and 4 * ni * njh * 2 * nr == LANES
    C = ni * njh * LANES
    coef = jnp.repeat(cell_coef, nr, axis=2)
    extra = jnp.stack([lax.rsqrt(coef), coef], 2)
    start = jnp.concatenate(
        [jnp.transpose(right_side, (1, 2, 0, 3)), extra, jnp.zeros((X, Y, D - Q - 2, lanes), F32)], 2)
    def padded(m):
        return jnp.pad(m, ((0, D - Q), (0, D - Q)))

    zero = jnp.zeros((D, D), F32)

    def both(a, b, c, d):
        return jnp.concatenate([jnp.concatenate([a, b], 1), jnp.concatenate([c, d], 1)], 0)

    m = padded(cell_matrix)
    f = [-padded(face_coupling[d]) for d in range(3)]
    ft = [x.T for x in f]
    mats = jnp.stack([
        both(m, zero, zero, m),
        both(zero, f[2], ft[2], zero),
        both(zero, ft[2], f[2], zero),
        both(f[0], zero, zero, f[0]),
        both(ft[0], zero, zero, ft[0]),
        both(f[1], zero, zero, f[1]),
        both(ft[1], zero, zero, ft[1]),
    ]).astype(BF16)
    half = njh * LANES
    V = pltpu.VMEM
    A = Q // 16 * 16
    assert Q == A + 1
    whole = (8, D, C)
    scratch = [
        V(whole, F32), V((2, *whole), F32), V(whole, F32), V(whole, BF16), V(whole, BF16), V(whole, BF16),
        V(whole, BF16), V(whole, BF16), V(whole, BF16),
        V((8, 2, 4, A, half), BF16), V((8, 2, 16, half), BF16),
        V((8, 2, 4, D, LANES), BF16), V((8, 2, D, LANES), BF16),
        V((2, 16, half), BF16), V((2, 4, D, LANES), BF16), V((2, D, LANES), BF16),
        V((2, 4, A, half), BF16), V((2, 4, 8, half), F32), V((4, D, half), BF16),
        V((4, 4, D, LANES), F32), V((2, 4, D, LANES), BF16), V((8, D, LANES), F32),
        V((4, A, half), BF16), V((4, D, half), BF16),
        V((4, D, LANES), F32), V((4, D, LANES), BF16), V((D, LANES), F32),
        V((8 * D, 8 * Q), BF16), V((8 * D, 8 * D), BF16),
        pltpu.SemaphoreType.DMA((96,)), pltpu.SemaphoreType.DMA((96,)),
    ]
    vmem = pl.BlockSpec(memory_space=pltpu.VMEM)
    sol, res = pl.pallas_call(
        functools.partial(kernel, sizes, (D, Q, nr, ni, njh)),
        out_shape=[jax.ShapeDtypeStruct((X, Y, D, lanes), F32)] * 2,
        in_specs=[vmem] * 3,
        out_specs=[vmem] * 2,
        scratch_shapes=scratch,
        compiler_params=pltpu.CompilerParams(
            collective_id=0, has_side_effects=True, vmem_limit_bytes=60 * 1024 * 1024),
    )(start, patch_inverse, mats)
    return tuple(jnp.transpose(x[:, :, :Q], (2, 0, 1, 3)) for x in (sol, res))


def solution(mesh):
    sizes = tuple(mesh.shape[a] for a in AXES)
    placed = (P(None, "gx", "gy", "gz"), P("gx", "gy", "gz"), P(), P(), P())
    return jax.shard_map(
        functools.partial(on_device, sizes),
        mesh=mesh,
        in_specs=placed,
        out_specs=(P(None, "gx", "gy", "gz"), P(None, "gx", "gy", "gz")),
        check_vma=False,
    )
```
